32 devices in a mesh: groups: 1, row: 4 (over z), col: 4 (over y, x), ksplit: 2 (over core).
Axes of the slice: x: 2, y: 2, z: 4, core: 2. Of those that a mesh axis runs over, the one named last changes fastest.
Arguments:
- pair_state: bfloat16 [128, 128, 128], P(('groups', 'row'), ('col', 'ksplit')), may hold values from -6 to 6
- residue_mask: int32 [128], P('groups'), may hold values 0 or 1
- input_gain: float32 [128], replicated, may hold values from 0.1 to 1.9
- input_shift: float32 [128], replicated, may hold values from -3 to 3
- left_right: bfloat16 [128, 512], replicated, may hold values from -0.5 to 0.5
- output_gate: bfloat16 [128, 128], replicated, may hold values from -0.5 to 0.5
- final_gain: float32 [128], replicated, may hold values from 0.1 to 1.9
- final_shift: float32 [128], replicated, may hold values from -3 to 3
- output_weight: bfloat16 [128, 128], replicated, may hold values from -0.5 to 0.5
Outputs:
- pair_update: bfloat16 [128, 128, 128], P(('groups', 'row'), ('col', 'ksplit'))
The draws below stay inside these ranges and needn't reach their ends.
All inputs are finite; a program needn't handle non-finite values.
Results may differ from the reference program's by a relative error of at most 0.0053.
Values may be sent and summed in bfloat16 or wider, within the bound.
A program may use at most 64 MiB of HBM per device.

```python
import jax
import jax.numpy as jnp
from jax import lax

C = 128
H = 128
N = 128
N_ROW = 4


def plant(entries, rng, smallest, top_value):
    longest = entries.shape.index(max(entries.shape))
    spots = []
    for shift in (0, 1):
        where = [jax.random.randint(jax.random.fold_in(rng, axis), (), 0, length) for axis, length in enumerate(entries.shape)]
        where[longest] = (where[longest] + shift) % entries.shape[longest]
        spots.append(tuple(where))
    return entries.at[spots[0]].set(smallest).at[spots[1]].set(top_value)


def shard_levels(rng, dims, split, smallest, largest):
    level, own = 1.0, jax.random.fold_in(rng, 6)
    for dim, parts in split:
        heights = jnp.exp(jax.random.uniform(jax.random.fold_in(own, dim), (parts,), jnp.float32, smallest / len(split), largest / len(split)))
        level = level * jnp.repeat(heights, dims[dim] // parts).reshape([-1 if axis == dim else 1 for axis in range(len(dims))])
    return level


def scatter_about(own_key, shape, scale, most, pieces=(), held_as=jnp.bfloat16):
    loudness = shard_levels(own_key, shape, pieces, -0.22, 0.18) if pieces else 1.0
    entries = jax.random.normal(own_key, shape, jnp.float32) * scale * loudness
    return jnp.minimum(jnp.maximum(entries, -most), most).astype(held_as)


def setup_inputs(seed: int = 0, part: int = 0) -> dict:
    seeds = jax.random.split(jax.random.key(seed), 10)
    own_keys = jax.random.split(jax.random.fold_in(seeds[9], part), 10)
    return {
        "pair_state": scatter_about(own_keys[0], (N, N, C), 1.0, 6.0, ((0, 4), (1, 8))),
        "residue_mask": plant((jax.random.randint(own_keys[1], (N,), 0, 4) < 3).astype(jnp.int32), jax.random.fold_in(own_keys[1], 1), 0, 1),
        "input_gain": jnp.clip(1.0 + 0.18 * jax.random.normal(seeds[2], (C,), jnp.float32), 0.1, 1.9),
        "input_shift": scatter_about(seeds[3], (C,), 0.5, 3.0, (), jnp.float32),
        "left_right": scatter_about(seeds[4], (C, 4 * H), C ** -0.5, 0.5),
        "output_gate": scatter_about(seeds[5], (C, C), C ** -0.5, 0.5),
        "final_gain": jnp.clip(1.0 + 0.18 * jax.random.normal(seeds[6], (H,), jnp.float32), 0.1, 1.9),
        "final_shift": scatter_about(seeds[7], (H,), 0.5, 3.0, (), jnp.float32),
        "output_weight": scatter_about(seeds[8], (H, C), H ** -0.5, 0.5),
    }


def norm_last(data, norm_gain, norm_shift):
    average = lax.optimization_barrier(jnp.mean(data, axis=-1, keepdims=True))
    centred = data - average
    spread = lax.optimization_barrier(jnp.mean(centred * centred, axis=-1, keepdims=True))
    return centred * lax.rsqrt(spread + 1e-05) * norm_gain + norm_shift

def reference(pair_state, residue_mask, input_gain, input_shift, left_right, output_gate, final_gain, final_shift, output_weight):
    live_rows = residue_mask.astype(jnp.float32)
    block_rows = N // N_ROW
    blocks_state = pair_state.reshape(N_ROW, block_rows, N, C)
    blocks_live = live_rows.reshape(N_ROW, block_rows)

    def one_block(pair):
        state_block, live_block = pair
        normed_block = norm_last(state_block.astype(jnp.float32), input_gain, input_shift).astype(jnp.bfloat16)
        flat_block = normed_block.reshape(block_rows * N, C)
        live_mask = (live_block[:, None] * live_rows[None, :])[:, :, None]
        left_proj = jnp.dot(flat_block, left_right[:, :2 * H], preferred_element_type=jnp.float32).reshape(block_rows, N, 2 * H)
        left_block = (live_mask * jax.nn.sigmoid(left_proj[:, :, H:]) * left_proj[:, :, :H]).astype(jnp.bfloat16)
        right_proj = jnp.dot(flat_block, left_right[:, 2 * H:], preferred_element_type=jnp.float32).reshape(block_rows, N, 2 * H)
        right_block = (live_mask * jax.nn.sigmoid(right_proj[:, :, H:]) * right_proj[:, :, :H]).astype(jnp.bfloat16)
        return (normed_block, left_block, right_block)
    normed_blocks, left_blocks, right_blocks = lax.map(one_block, (blocks_state, blocks_live))
    normed_in = normed_blocks.reshape(N, N, C)
    left_side = left_blocks.reshape(N, N, H)
    right_side = right_blocks.reshape(N, N, H)
    flat_rows = normed_in.reshape(N * N, C)
    left_major = jnp.transpose(left_side, (2, 0, 1))
    right_major = jnp.transpose(right_side, (2, 0, 1))

    def one_channel(pair):
        lhs, rhs = pair
        return jnp.dot(lhs.astype(jnp.float32), rhs.astype(jnp.float32).T, precision=lax.Precision.HIGHEST)
    mixed_all = lax.map(one_channel, (left_major, right_major))
    mixed_last = jnp.transpose(mixed_all, (1, 2, 0))
    normed_out = norm_last(mixed_last, final_gain, final_shift).astype(jnp.bfloat16)
    gate_values = jax.nn.sigmoid(jnp.dot(flat_rows, output_gate, preferred_element_type=jnp.float32))
    projected_out = jnp.dot(normed_out.reshape(N * N, H), output_weight, preferred_element_type=jnp.float32)
    return (gate_values * projected_out).reshape(N, N, C).astype(jnp.bfloat16)
```

```python
import functools

import jax
import jax.numpy as jnp
from jax import lax
from jax.experimental import pallas as pl
from jax.experimental.pallas import tpu as pltpu
from jax.sharding import PartitionSpec as P

MESH = pl.DeviceIdType.MESH
LANES = 128
F32 = jnp.float32
BF16 = jnp.bfloat16
BACK = jnp.bfloat16


def norm_rows(data, gain, shift):
    average = jnp.mean(data, axis=-1, keepdims=True)
    centred = data - average
    spread = jnp.mean(centred * centred, axis=-1, keepdims=True)
    return centred * lax.rsqrt(spread + 1e-05) * gain + shift


def swap_blocks(parts, width):
    count = len(parts)
    lane_block = lax.broadcasted_iota(jnp.int32, parts[0].shape, 1) // width
    parts = list(parts)
    step = count // 2
    while step:
        upper = (lane_block & step) != 0
        for low in range(count):
            if low & step:
                continue
            first, second = parts[low], parts[low + step]
            parts[low] = jnp.where(upper, pltpu.roll(second, step * width, 1), first)
            parts[low + step] = jnp.where(
                upper, second, pltpu.roll(first, LANES - step * width, 1)
            )
        step //= 2
    return parts


def kernel(
    sizes,
    state_ref,
    mask_scalars,
    mask_ref,
    input_gain,
    input_shift,
    left_right,
    output_gate,
    final_gain,
    final_shift,
    output_weight,
    out_ref,
    normed_buf,
    gate_buf,
    left_stage,
    right_stage,
    send,
    recv,
    back,
    home,
    send_sem,
    recv_sem,
    back_sem,
    home_sem,
):
    row_count, col_count, split_count, tile_rows, tile_cols, channels, hidden = sizes
    plane = col_count * split_count
    devices = row_count * plane
    blocks = LANES // tile_rows
    my_row = lax.axis_index("row")
    my_plane = lax.axis_index("col") * split_count + lax.axis_index("ksplit")
    me = my_row * plane + my_plane

    def place(index):
        within = lax.rem(index, plane)
        return {
            "row": index // plane,
            "col": within // split_count,
            "ksplit": lax.rem(within, split_count),
        }

    barrier = pltpu.get_barrier_semaphore()

    def greet(step, carry):
        pl.semaphore_signal(
            barrier, inc=1, device_id=place(lax.rem(me + step, devices)), device_id_type=MESH
        )
        return carry

    lax.fori_loop(1, devices, greet, 0)

    positions = tile_rows * tile_cols
    state = state_ref[...].astype(F32).reshape(positions, channels)
    normed = norm_rows(state, input_gain[...], input_shift[...]).astype(BF16)
    normed_buf[...] = normed.astype(F32)
    weights = jnp.transpose(left_right[...].astype(F32)).astype(BF16)

    lane_block = lax.broadcasted_iota(jnp.int32, (tile_rows, LANES), 1) // tile_rows
    mask_rows = jnp.broadcast_to(mask_ref[...].astype(F32), (tile_rows, LANES))
    row_live = mask_rows
    turn = lax.rem(lane_block - my_row + row_count, row_count)
    for shift in range(1, blocks):
        row_live = jnp.where(turn == shift, pltpu.roll(mask_rows, shift * tile_rows, 1), row_live)

    for quarter in range(tile_cols // blocks):
        rows = []
        col_live = jnp.zeros((tile_rows, LANES), F32)
        for inner in range(blocks):
            k = quarter * blocks + inner
            rows.append(normed_buf[pl.ds(k, tile_rows, stride=tile_cols), :])
            alive = mask_scalars[my_plane * tile_cols + k].astype(F32)
            col_live = jnp.where(lane_block == inner, alive, col_live)
        live = row_live * col_live
        packed = jnp.concatenate(rows, axis=0).astype(BF16)
        projected = lax.dot_general(
            weights, packed, (((1,), (1,)), ((), ())), preferred_element_type=F32
        )
        for side, stage in ((0, left_stage), (1, right_stage)):
            parts = []
            for block in range(blocks):
                at = side * 2 * hidden + block * devices
                value = projected[at : at + devices]
                gate = projected[at + hidden : at + hidden + devices]
                parts.append(live[:devices] * jax.nn.sigmoid(gate) * value)
            swapped = swap_blocks(parts, tile_rows)
            for inner in range(blocks):
                k = quarter * blocks + inner
                stage[pl.ds(k, devices, stride=tile_cols), :] = swapped[inner]
    send[:, 0] = left_stage[...].reshape(devices, tile_cols, LANES).astype(BF16)
    send[:, 1] = right_stage[...].reshape(devices, tile_cols, LANES).astype(BF16)

    pl.semaphore_wait(barrier, devices - 1)

    def outgoing(target):
        return pltpu.make_async_remote_copy(
            src_ref=send.at[target],
            dst_ref=recv.at[me],
            send_sem=send_sem.at[target],
            recv_sem=recv_sem.at[me],
            device_id=place(target),
            device_id_type=MESH,
        )

    def incoming(source):
        return pltpu.make_async_remote_copy(
            src_ref=send.at[source],
            dst_ref=recv.at[source],
            send_sem=send_sem.at[source],
            recv_sem=recv_sem.at[source],
            device_id=place(source),
            device_id_type=MESH,
        )

    def start_first(step, carry):
        outgoing(lax.rem(me + step, devices)).start()
        return carry

    lax.fori_loop(1, devices, start_first, 0)
    recv[me] = send[me]
    gates = jnp.dot(normed, output_gate[...], preferred_element_type=F32)
    gate_buf[...] = jax.nn.sigmoid(gates).reshape(tile_rows, tile_cols, channels)

    def wait_first(step, carry):
        incoming(lax.rem(me + devices - step, devices)).wait_recv()
        return carry

    lax.fori_loop(1, devices, wait_first, 0)

    def gathered(side, row):
        return recv[row * plane : (row + 1) * plane, side].reshape(plane * tile_cols, LANES)

    rights = [gathered(1, row) for row in range(row_count)]
    rights = jnp.concatenate(rights, axis=1)
    half_bit = (lax.broadcasted_iota(jnp.int32, (tile_cols, LANES), 1) // tile_cols) & 1
    for row in range(row_count):
        lefts = jnp.transpose(gathered(0, row).astype(F32)).astype(BF16)
        products = jnp.dot(lefts, rights, preferred_element_type=F32)
        for other in range(row_count):
            piece = products[:, other * LANES : (other + 1) * LANES]
            mixed = piece[:tile_rows]
            for block in range(1, blocks):
                mixed = jnp.where(
                    lane_block == block, piece[block * tile_rows : (block + 1) * tile_rows], mixed
                )
            upper, lower = mixed[:tile_cols], mixed[tile_cols:]
            first = jnp.where(half_bit == 0, upper, pltpu.roll(lower, tile_cols, 1))
            second = jnp.where(half_bit == 1, lower, pltpu.roll(upper, LANES - tile_cols, 1))
            target = row * plane + other * 2
            back[target] = first.astype(BACK)
            back[target + 1] = second.astype(BACK)

    def returning(target):
        return pltpu.make_async_remote_copy(
            src_ref=back.at[target],
            dst_ref=home.at[me],
            send_sem=back_sem.at[target],
            recv_sem=home_sem.at[me],
            device_id=place(target),
            device_id_type=MESH,
        )

    def coming_home(source):
        return pltpu.make_async_remote_copy(
            src_ref=back.at[source],
            dst_ref=home.at[source],
            send_sem=back_sem.at[source],
            recv_sem=home_sem.at[source],
            device_id=place(source),
            device_id_type=MESH,
        )

    def start_second(step, carry):
        returning(lax.rem(me + step, devices)).start()
        return carry

    lax.fori_loop(1, devices, start_second, 0)
    home[me] = back[me]

    def wait_second(step, carry):
        coming_home(lax.rem(me + devices - step, devices)).wait_recv()
        return carry

    lax.fori_loop(1, devices, wait_second, 0)

    left_stage[...] = home[...].astype(F32).reshape(devices * tile_cols, LANES)
    for group in range(tile_cols // blocks):
        rows = [
            left_stage[pl.ds(group * blocks + inner, devices, stride=tile_cols), :]
            for inner in range(blocks)
        ]
        turned = jnp.transpose(jnp.concatenate(rows, axis=0))
        parts = [turned[b * tile_rows : (b + 1) * tile_rows] for b in range(blocks)]
        together = jnp.concatenate(swap_blocks(parts, devices), axis=0)
        normed_out = norm_rows(together, final_gain[...], final_shift[...]).astype(BF16)
        projected_out = jnp.dot(normed_out, output_weight[...], preferred_element_type=F32)
        for inner in range(blocks):
            for half in range(2):
                i = half * tile_cols + group * blocks + inner
                at = inner * tile_rows + half * tile_cols
                out_ref[i] = (gate_buf[i] * projected_out[at : at + tile_cols]).astype(BF16)

    def drain(step, carry):
        target = lax.rem(me + step, devices)
        outgoing(target).wait_send()
        returning(target).wait_send()
        return carry

    lax.fori_loop(1, devices, drain, 0)


def fused(sizes, *arrays):
    row_count, col_count, split_count, tile_rows, tile_cols, channels, hidden = sizes
    devices = row_count * col_count * split_count
    state, mask, gain_in, shift_in, weights, gate, gain_out, shift_out, weight_out = arrays
    vmem = pl.BlockSpec(memory_space=pltpu.VMEM)
    smem = pl.BlockSpec(memory_space=pltpu.SMEM)
    return pl.pallas_call(
        functools.partial(kernel, sizes),
        out_shape=jax.ShapeDtypeStruct(state.shape, BF16),
        in_specs=[vmem, smem] + [vmem] * 8,
        out_specs=vmem,
        scratch_shapes=[
            pltpu.VMEM((tile_rows * tile_cols, channels), F32),
            pltpu.VMEM((tile_rows, tile_cols, channels), F32),
            pltpu.VMEM((devices * tile_cols, LANES), F32),
            pltpu.VMEM((devices * tile_cols, LANES), F32),
            pltpu.VMEM((devices, 2, tile_cols, LANES), BF16),
            pltpu.VMEM((devices, 2, tile_cols, LANES), BF16),
            pltpu.VMEM((devices, tile_cols, LANES), BACK),
            pltpu.VMEM((devices, tile_cols, LANES), BACK),
            pltpu.SemaphoreType.DMA((devices,)),
            pltpu.SemaphoreType.DMA((devices,)),
            pltpu.SemaphoreType.DMA((devices,)),
            pltpu.SemaphoreType.DMA((devices,)),
        ],
        compiler_params=pltpu.CompilerParams(collective_id=0, has_side_effects=True),
    )(
        state,
        mask,
        mask[None],
        gain_in[None],
        shift_in[None],
        weights,
        gate,
        gain_out[None],
        shift_out[None],
        weight_out,
    )


def update(*arrays):
    state, mask, weight_out = arrays[0], arrays[1], arrays[8]
    tile_rows, tile_cols, channels = state.shape
    hidden = weight_out.shape[0]
    row_count, col_count = lax.axis_size("row"), lax.axis_size("col")
    split_count = lax.axis_size("ksplit")
    devices = row_count * col_count * split_count
    fits = (
        channels == LANES
        and hidden == LANES
        and mask.shape[0] == LANES
        and row_count * tile_rows == LANES
        and devices == tile_rows
        and tile_rows == 2 * tile_cols
        and tile_cols % 16 == 0
    )
    if fits:
        sizes = (row_count, col_count, split_count, tile_rows, tile_cols, channels, hidden)
        return fused(sizes, *arrays)
    return body(*arrays)


def norm_over(data, norm_gain, norm_shift, over_axis):
    average = jnp.mean(data, axis=over_axis, keepdims=True)
    centred = data - average
    spread = jnp.mean(centred * centred, axis=over_axis, keepdims=True)
    return centred * lax.rsqrt(spread + 1e-05) * norm_gain + norm_shift


def gated_side(normed_in, weights, live_mask, hidden):
    values = jnp.einsum(
        "ikc,ch->hik", normed_in, weights[:, :hidden], preferred_element_type=jnp.float32
    )
    gates = jnp.einsum(
        "ikc,ch->hik", normed_in, weights[:, hidden:], preferred_element_type=jnp.float32
    )
    return (live_mask * jax.nn.sigmoid(gates) * values).astype(jnp.bfloat16)


def contract_parts(left_parts, right_parts, row_count, col_count):
    count_items = left_parts.shape[2]
    tile_rows = left_parts.shape[3]
    tile_cols = left_parts.shape[4]

    def assemble(parts):
        return parts.transpose(2, 0, 3, 1, 4).reshape(
            count_items, row_count * tile_rows, col_count * tile_cols
        )

    products = jnp.einsum(
        "cik,cjk->cij",
        assemble(left_parts),
        assemble(right_parts),
        preferred_element_type=jnp.float32,
    )
    returned = products.reshape(count_items, row_count, tile_rows, col_count, tile_cols)
    return returned.transpose(1, 3, 0, 2, 4)


def body(
    pair_state,
    residue_mask,
    input_gain,
    input_shift,
    left_right,
    output_gate,
    final_gain,
    final_shift,
    output_weight,
):
    tile_rows, tile_cols, channels = pair_state.shape
    hidden = output_weight.shape[0]
    normed_in = norm_over(pair_state.astype(jnp.float32), input_gain, input_shift, 2).astype(
        jnp.bfloat16
    )
    row_start = lax.axis_index("row") * tile_rows
    col_start = lax.axis_index(("col", "ksplit")) * tile_cols
    row_live = lax.dynamic_slice_in_dim(residue_mask, row_start, tile_rows).astype(jnp.float32)
    col_live = lax.dynamic_slice_in_dim(residue_mask, col_start, tile_cols).astype(jnp.float32)
    live_mask = row_live[:, None] * col_live[None, :]
    left_side = gated_side(normed_in, left_right[:, : 2 * hidden], live_mask, hidden)
    right_side = gated_side(normed_in, left_right[:, 2 * hidden :], live_mask, hidden)
    devices_all = lax.axis_size(("row", "col", "ksplit"))
    row_count = lax.axis_size("row")
    col_count = devices_all // row_count
    per_device = hidden // devices_all
    grouped_left = left_side.reshape(devices_all, per_device, tile_rows, tile_cols)
    grouped_right = right_side.reshape(devices_all, per_device, tile_rows, tile_cols)
    left_parts = lax.all_to_all(
        grouped_left, ("row", "col", "ksplit"), split_axis=0, concat_axis=0, tiled=True
    )
    right_parts = lax.all_to_all(
        grouped_right, ("row", "col", "ksplit"), split_axis=0, concat_axis=0, tiled=True
    )
    count_items = left_parts.shape[1]
    shaped_left = left_parts.reshape(row_count, col_count, count_items, tile_rows, tile_cols)
    shaped_right = right_parts.reshape(row_count, col_count, count_items, tile_rows, tile_cols)
    returned = contract_parts(shaped_left, shaped_right, row_count, col_count)
    returned = returned.reshape(devices_all, count_items, tile_rows, tile_cols)
    received = lax.all_to_all(
        returned, ("row", "col", "ksplit"), split_axis=0, concat_axis=0, tiled=True
    )
    mixed_tile = received.reshape(hidden, tile_rows, tile_cols)
    normed_out = norm_over(
        mixed_tile, final_gain[:, None, None], final_shift[:, None, None], 0
    ).astype(jnp.bfloat16)
    projected_out = jnp.einsum(
        "hij,hc->ijc", normed_out, output_weight, preferred_element_type=jnp.float32
    )
    gate_values = jax.nn.sigmoid(
        jnp.einsum("ijc,cd->ijd", normed_in, output_gate, preferred_element_type=jnp.float32)
    )
    return (gate_values * projected_out).astype(jnp.bfloat16)


def solution(mesh):
    placed = (
        P(("groups", "row"), ("col", "ksplit"), None),
        P("groups"),
        P(),
        P(),
        P(),
        P(),
        P(),
        P(),
        P(),
    )
    return jax.shard_map(
        update,
        mesh=mesh,
        in_specs=placed,
        out_specs=P(("groups", "row"), ("col", "ksplit"), None),
        check_vma=False,
    )
```

```python
import functools

import jax
import jax.numpy as jnp
from jax import lax
from jax.experimental import pallas as pl
from jax.experimental.pallas import tpu as pltpu
from jax.sharding import PartitionSpec as P

MESH = pl.DeviceIdType.MESH
LANES = 128
F32 = jnp.float32
BF16 = jnp.bfloat16
BACK = jnp.bfloat16


def norm_rows(data, gain, shift):
    average = jnp.mean(data, axis=-1, keepdims=True)
    centred = data - average
    spread = jnp.mean(centred * centred, axis=-1, keepdims=True)
    return centred * lax.rsqrt(spread + 1e-05) * gain + shift


def swap_blocks(parts, width):
    count = len(parts)
    lane_block = lax.broadcasted_iota(jnp.int32, parts[0].shape, 1) // width
    parts = list(parts)
    step = count // 2
    while step:
        upper = (lane_block & step) != 0
        for low in range(count):
            if low & step:
                continue
            first, second = parts[low], parts[low + step]
            parts[low] = jnp.where(upper, pltpu.roll(second, step * width, 1), first)
            parts[low + step] = jnp.where(
                upper, second, pltpu.roll(first, LANES - step * width, 1)
            )
        step //= 2
    return parts


def kernel(sizes, *refs):
    row_count, col_count, split_count, tile_rows, tile_cols, channels, hidden = sizes
    hbm_inputs, out_ref, inputs = refs[:9], refs[9], refs[10:19]
    normed_buf, gate_buf, left_stage, right_stage = refs[19:23]
    left_send, right_send, left_recv, right_recv, back, home = refs[23:29]
    load_sem, left_out, left_in, right_out, right_in, back_out, back_in = refs[29:36]
    state_ref, mask_ref, input_gain, input_shift, left_right = inputs[:5]
    output_gate, final_gain, final_shift, output_weight = inputs[5:]
    plane = col_count * split_count
    devices = row_count * plane
    owners = devices // 2
    half_rows = row_count // 2
    blocks = LANES // tile_rows
    my_row = lax.axis_index("row")
    my_plane = lax.axis_index("col") * split_count + lax.axis_index("ksplit")
    me = my_row * plane + my_plane
    my_base = (my_row // half_rows) * owners
    my_group = lax.rem(me, owners)
    my_inner = lax.rem(my_row, half_rows)

    def place(index):
        within = lax.rem(index, plane)
        return {
            "row": index // plane,
            "col": within // split_count,
            "ksplit": lax.rem(within, split_count),
        }

    loads = [
        pltpu.make_async_copy(source, target, load_sem.at[at])
        for at, (source, target) in enumerate(zip(hbm_inputs, inputs))
    ]
    for load in loads:
        load.start()

    barrier = pltpu.get_barrier_semaphore()

    def greet(step, carry):
        pl.semaphore_signal(
            barrier, inc=1, device_id=place(lax.rem(me + step, devices)), device_id_type=MESH
        )
        return carry

    lax.fori_loop(1, devices, greet, 0)
    for load in loads:
        load.wait()

    positions = tile_rows * tile_cols
    state = state_ref[...].astype(F32).reshape(positions, channels)
    normed = norm_rows(state, input_gain[...], input_shift[...]).astype(BF16)
    normed_buf[...] = normed.astype(F32)
    weights = jnp.transpose(left_right[...].astype(F32)).astype(BF16)

    lane = lax.broadcasted_iota(jnp.int32, (1, LANES), 1)
    lane_block = lax.broadcasted_iota(jnp.int32, (tile_rows, LANES), 1) // tile_rows
    mask_line = mask_ref[...].astype(F32)
    mask_rows = jnp.broadcast_to(mask_line, (tile_rows, LANES))
    row_live = mask_rows
    turn = lax.rem(lane_block - my_row + row_count, row_count)
    for shift in range(1, blocks):
        row_live = jnp.where(turn == shift, pltpu.roll(mask_rows, shift * tile_rows, 1), row_live)

    for quarter in range(tile_cols // blocks):
        rows = []
        col_live = jnp.zeros((tile_rows, LANES), F32)
        for inner in range(blocks):
            k = quarter * blocks + inner
            rows.append(normed_buf[pl.ds(k, tile_rows, stride=tile_cols), :])
            alive = jnp.where(lane == my_plane * tile_cols + k, mask_line, 0.0)
            alive = jnp.sum(alive, axis=1, keepdims=True)
            col_live = jnp.where(lane_block == inner, alive, col_live)
        live = row_live * col_live
        packed = jnp.concatenate(rows, axis=0).astype(BF16)
        projected = lax.dot_general(
            weights, packed, (((1,), (1,)), ((), ())), preferred_element_type=F32
        )
        for side, stage in ((0, left_stage), (1, right_stage)):
            parts = []
            for block in range(blocks):
                at = side * 2 * hidden + block * tile_rows
                value = projected[at : at + tile_rows]
                gate = projected[at + hidden : at + hidden + tile_rows]
                parts.append(live * jax.nn.sigmoid(gate) * value)
            swapped = swap_blocks(parts, tile_rows)
            for inner in range(blocks):
                k = quarter * blocks + inner
                stage[pl.ds(k, tile_rows, stride=tile_cols), :] = swapped[inner]
    right_send[...] = right_stage[...].reshape(right_send.shape).astype(BF16)
    left_send[...] = left_stage[...].reshape(left_send.shape).astype(BF16)

    pl.semaphore_wait(barrier, devices - 1)

    def right_copy(target, source, arriving):
        row = source // plane
        return pltpu.make_async_remote_copy(
            src_ref=right_send.at[:, lax.rem(target, owners)],
            dst_ref=right_recv.at[:, row, lax.rem(source, plane)],
            send_sem=right_out.at[target],
            recv_sem=right_in.at[source],
            device_id=place(source if arriving else target),
            device_id_type=MESH,
        )

    def left_copy(target, source, arriving):
        row = lax.rem(source, owners) // plane
        return pltpu.make_async_remote_copy(
            src_ref=left_send.at[:, target],
            dst_ref=left_recv.at[:, row, lax.rem(source, plane)],
            send_sem=left_out.at[target],
            recv_sem=left_in.at[lax.rem(source, owners)],
            device_id=place(my_base + (lax.rem(source, owners) if arriving else target)),
            device_id_type=MESH,
        )

    def back_copy(target, source, arriving):
        return pltpu.make_async_remote_copy(
            src_ref=back.at[target],
            dst_ref=home.at[source],
            send_sem=back_out.at[target],
            recv_sem=back_in.at[source],
            device_id=place(my_base + (source if arriving else target)),
            device_id_type=MESH,
        )

    far_base = owners - my_base

    def send_far(step, carry):
        right_copy(far_base + lax.rem(my_group + step, owners), me, False).start()
        return carry

    def send_near(step, carry):
        target = lax.rem(my_group + step, owners)
        right_copy(my_base + target, me, False).start()
        left_copy(target, me, False).start()
        return carry

    lax.fori_loop(0, owners, send_far, 0)
    lax.fori_loop(1, owners, send_near, 0)
    right_recv[:, my_row, my_plane] = right_send[:, my_group]
    left_recv[:, my_inner, my_plane] = left_send[:, my_group]
    gates = jnp.dot(normed, output_gate[...], preferred_element_type=F32)
    gate_buf[...] = jax.nn.sigmoid(gates)

    def wait_near(step, carry):
        source = lax.rem(my_group + owners - step, owners)
        left_copy(source, source, True).wait_recv()
        right_copy(my_base + source, my_base + source, True).wait_recv()
        return carry

    def wait_far(step, carry):
        source = far_base + lax.rem(my_group + owners - step, owners)
        right_copy(source, source, True).wait_recv()
        return carry

    lax.fori_loop(1, owners, wait_near, 0)
    lax.fori_loop(0, owners, wait_far, 0)

    depth = plane * tile_cols
    rights = [
        jnp.concatenate(
            [right_recv[bit, row].reshape(depth, LANES) for row in range(row_count)], axis=1
        )
        for bit in range(2)
    ]
    half_bit = (lax.broadcasted_iota(jnp.int32, (tile_rows, LANES), 1) // tile_cols) & 1
    for inner in range(half_rows):
        products = []
        for bit in range(2):
            lefts = left_recv[bit, inner].reshape(depth, LANES)
            lefts = jnp.transpose(lefts.astype(F32)).astype(BF16)
            products.append(jnp.dot(lefts, rights[bit], preferred_element_type=F32))
        for other in range(row_count):
            mixed = []
            for product in products:
                piece = product[:, other * LANES : (other + 1) * LANES]
                chosen = piece[:tile_rows]
                for block in range(1, blocks):
                    chosen = jnp.where(
                        lane_block == block,
                        piece[block * tile_rows : (block + 1) * tile_rows],
                        chosen,
                    )
                mixed.append(chosen)
            first = jnp.where(half_bit == 0, mixed[0], pltpu.roll(mixed[1], tile_cols, 1))
            second = jnp.where(
                half_bit == 1, mixed[1], pltpu.roll(mixed[0], LANES - tile_cols, 1)
            )
            target = inner * plane + other * 2
            back[target] = first.astype(BACK)
            back[target + 1] = second.astype(BACK)

    def send_back(step, carry):
        back_copy(lax.rem(my_group + step, owners), my_group, False).start()
        return carry

    def wait_back(step, carry):
        source = lax.rem(my_group + owners - step, owners)
        back_copy(source, source, True).wait_recv()
        return carry

    lax.fori_loop(1, owners, send_back, 0)
    home[my_group] = back[my_group]
    lax.fori_loop(1, owners, wait_back, 0)

    left_stage[...] = home[...].astype(F32).reshape(owners * tile_rows, LANES)
    step_rows = LANES // tile_cols
    for group in range(tile_rows // step_rows):
        rows = [
            left_stage[pl.ds(group * step_rows + at, owners, stride=tile_rows), :]
            for at in range(step_rows)
        ]
        turned = jnp.transpose(jnp.concatenate(rows, axis=0))
        parts = [turned[b * tile_cols : (b + 1) * tile_cols] for b in range(step_rows)]
        together = jnp.concatenate(swap_blocks(parts, owners), axis=0)
        normed_out = norm_rows(together, final_gain[...], final_shift[...]).astype(BF16)
        projected_out = jnp.dot(normed_out, output_weight[...], preferred_element_type=F32)
        gated = gate_buf[group * LANES : (group + 1) * LANES] * projected_out
        out_ref[group * step_rows : (group + 1) * step_rows] = gated.reshape(
            step_rows, tile_cols, channels
        ).astype(BF16)

    def drain_near(step, carry):
        target = lax.rem(my_group + step, owners)
        right_copy(my_base + target, me, False).wait_send()
        left_copy(target, me, False).wait_send()
        back_copy(target, my_group, False).wait_send()
        return carry

    def drain_far(step, carry):
        right_copy(far_base + lax.rem(my_group + step, owners), me, False).wait_send()
        return carry

    lax.fori_loop(1, owners, drain_near, 0)
    lax.fori_loop(0, owners, drain_far, 0)


def fused(sizes, *arrays):
    row_count, col_count, split_count, tile_rows, tile_cols, channels, hidden = sizes
    plane = col_count * split_count
    devices = row_count * plane
    owners = devices // 2
    state, *lines, weights, gate, gain_out, shift_out, weight_out = arrays
    lines = [line[None] for line in lines]
    operands = [state, *lines, weights, gate, gain_out[None], shift_out[None], weight_out]
    flat = (tile_rows * tile_cols, LANES)
    tile = (tile_cols, LANES)
    counts = (len(operands), owners, owners, devices, devices, owners, owners)
    return pl.pallas_call(
        functools.partial(kernel, sizes),
        out_shape=jax.ShapeDtypeStruct(state.shape, BF16),
        in_specs=[pl.BlockSpec(memory_space=pl.ANY)] * len(operands),
        out_specs=pl.BlockSpec(memory_space=pltpu.VMEM),
        scratch_shapes=[pltpu.VMEM(item.shape, item.dtype) for item in operands]
        + [pltpu.VMEM(flat, F32)] * 4
        + [pltpu.VMEM((2, owners) + tile, BF16)] * 2
        + [
            pltpu.VMEM((2, row_count // 2, plane) + tile, BF16),
            pltpu.VMEM((2, row_count, plane) + tile, BF16),
            pltpu.VMEM((owners, tile_rows, LANES), BACK),
            pltpu.VMEM((owners, tile_rows, LANES), BACK),
        ]
        + [pltpu.SemaphoreType.DMA((count,)) for count in counts],
        compiler_params=pltpu.CompilerParams(collective_id=0, has_side_effects=True),
    )(*operands)


def update(*arrays):
    state, mask, weight_out = arrays[0], arrays[1], arrays[8]
    tile_rows, tile_cols, channels = state.shape
    hidden = weight_out.shape[0]
    row_count, col_count = lax.axis_size("row"), lax.axis_size("col")
    split_count = lax.axis_size("ksplit")
    devices = row_count * col_count * split_count
    fits = (
        channels == LANES
        and hidden == LANES
        and mask.shape[0] == LANES
        and row_count * tile_rows == LANES
        and devices == tile_rows
        and row_count % 2 == 0
        and devices // 2 == tile_cols
        and tile_rows == 2 * tile_cols
        and tile_cols % 16 == 0
    )
    if fits:
        sizes = (row_count, col_count, split_count, tile_rows, tile_cols, channels, hidden)
        return fused(sizes, *arrays)
    return body(*arrays)


def norm_over(data, norm_gain, norm_shift, over_axis):
    average = jnp.mean(data, axis=over_axis, keepdims=True)
    centred = data - average
    spread = jnp.mean(centred * centred, axis=over_axis, keepdims=True)
    return centred * lax.rsqrt(spread + 1e-05) * norm_gain + norm_shift


def gated_side(normed_in, weights, live_mask, hidden):
    values = jnp.einsum(
        "ikc,ch->hik", normed_in, weights[:, :hidden], preferred_element_type=jnp.float32
    )
    gates = jnp.einsum(
        "ikc,ch->hik", normed_in, weights[:, hidden:], preferred_element_type=jnp.float32
    )
    return (live_mask * jax.nn.sigmoid(gates) * values).astype(jnp.bfloat16)


def contract_parts(left_parts, right_parts, row_count, col_count):
    count_items = left_parts.shape[2]
    tile_rows = left_parts.shape[3]
    tile_cols = left_parts.shape[4]

    def assemble(parts):
        return parts.transpose(2, 0, 3, 1, 4).reshape(
            count_items, row_count * tile_rows, col_count * tile_cols
        )

    products = jnp.einsum(
        "cik,cjk->cij",
        assemble(left_parts),
        assemble(right_parts),
        preferred_element_type=jnp.float32,
    )
    returned = products.reshape(count_items, row_count, tile_rows, col_count, tile_cols)
    return returned.transpose(1, 3, 0, 2, 4)


def body(
    pair_state,
    residue_mask,
    input_gain,
    input_shift,
    left_right,
    output_gate,
    final_gain,
    final_shift,
    output_weight,
):
    tile_rows, tile_cols, channels = pair_state.shape
    hidden = output_weight.shape[0]
    normed_in = norm_over(pair_state.astype(jnp.float32), input_gain, input_shift, 2).astype(
        jnp.bfloat16
    )
    row_start = lax.axis_index("row") * tile_rows
    col_start = lax.axis_index(("col", "ksplit")) * tile_cols
    row_live = lax.dynamic_slice_in_dim(residue_mask, row_start, tile_rows).astype(jnp.float32)
    col_live = lax.dynamic_slice_in_dim(residue_mask, col_start, tile_cols).astype(jnp.float32)
    live_mask = row_live[:, None] * col_live[None, :]
    left_side = gated_side(normed_in, left_right[:, : 2 * hidden], live_mask, hidden)
    right_side = gated_side(normed_in, left_right[:, 2 * hidden :], live_mask, hidden)
    devices_all = lax.axis_size(("row", "col", "ksplit"))
    row_count = lax.axis_size("row")
    col_count = devices_all // row_count
    per_device = hidden // devices_all
    grouped_left = left_side.reshape(devices_all, per_device, tile_rows, tile_cols)
    grouped_right = right_side.reshape(devices_all, per_device, tile_rows, tile_cols)
    left_parts = lax.all_to_all(
        grouped_left, ("row", "col", "ksplit"), split_axis=0, concat_axis=0, tiled=True
    )
    right_parts = lax.all_to_all(
        grouped_right, ("row", "col", "ksplit"), split_axis=0, concat_axis=0, tiled=True
    )
    count_items = left_parts.shape[1]
    shaped_left = left_parts.reshape(row_count, col_count, count_items, tile_rows, tile_cols)
    shaped_right = right_parts.reshape(row_count, col_count, count_items, tile_rows, tile_cols)
    returned = contract_parts(shaped_left, shaped_right, row_count, col_count)
    returned = returned.reshape(devices_all, count_items, tile_rows, tile_cols)
    received = lax.all_to_all(
        returned, ("row", "col", "ksplit"), split_axis=0, concat_axis=0, tiled=True
    )
    mixed_tile = received.reshape(hidden, tile_rows, tile_cols)
    normed_out = norm_over(
        mixed_tile, final_gain[:, None, None], final_shift[:, None, None], 0
    ).astype(jnp.bfloat16)
    projected_out = jnp.einsum(
        "hij,hc->ijc", normed_out, output_weight, preferred_element_type=jnp.float32
    )
    gate_values = jax.nn.sigmoid(
        jnp.einsum("ijc,cd->ijd", normed_in, output_gate, preferred_element_type=jnp.float32)
    )
    return (gate_values * projected_out).astype(jnp.bfloat16)


def solution(mesh):
    placed = (
        P(("groups", "row"), ("col", "ksplit"), None),
        P("groups"),
        P(),
        P(),
        P(),
        P(),
        P(),
        P(),
        P(),
    )
    return jax.shard_map(
        update,
        mesh=mesh,
        in_specs=placed,
        out_specs=P(("groups", "row"), ("col", "ksplit"), None),
        check_vma=False,
    )
```

```python
import functools

import jax
import jax.numpy as jnp
from jax import lax
from jax.experimental import pallas as pl
from jax.experimental.pallas import tpu as pltpu
from jax.sharding import PartitionSpec as P

MESH = pl.DeviceIdType.MESH
LANES = 128
F32 = jnp.float32
BF16 = jnp.bfloat16
BACK = jnp.bfloat16


def norm_rows(data, gain, shift):
    average = jnp.mean(data, axis=-1, keepdims=True)
    centred = data - average
    spread = jnp.mean(centred * centred, axis=-1, keepdims=True)
    return centred * lax.rsqrt(spread + 1e-05) * gain + shift


def swap_blocks(parts, width):
    count = len(parts)
    lane_block = lax.broadcasted_iota(jnp.int32, parts[0].shape, 1) // width
    parts = list(parts)
    step = count // 2
    while step:
        upper = (lane_block & step) != 0
        for low in range(count):
            if low & step:
                continue
            first, second = parts[low], parts[low + step]
            parts[low] = jnp.where(upper, pltpu.roll(second, step * width, 1), first)
            parts[low + step] = jnp.where(
                upper, second, pltpu.roll(first, LANES - step * width, 1)
            )
        step //= 2
    return parts


def kernel(sizes, *refs):
    row_count, col_count, split_count, tile_rows, tile_cols, channels, hidden = sizes
    hbm_inputs, out_ref, inputs = refs[:9], refs[9], refs[10:19]
    normed_buf, gate_buf, left_stage, right_stage = refs[19:23]
    left_send, right_send, left_recv, right_recv, back, home = refs[23:29]
    load_sem, left_out, left_in, right_out, right_in, back_out, back_in = refs[29:36]
    state_ref, mask_ref, input_gain, input_shift, left_right = inputs[:5]
    output_gate, final_gain, final_shift, output_weight = inputs[5:]
    plane = col_count * split_count
    devices = row_count * plane
    owners = devices // 2
    half_rows = row_count // 2
    blocks = LANES // tile_rows
    my_row = lax.axis_index("row")
    my_plane = lax.axis_index("col") * split_count + lax.axis_index("ksplit")
    me = my_row * plane + my_plane
    my_base = (my_row // half_rows) * owners
    my_group = lax.rem(me, owners)
    my_inner = lax.rem(my_row, half_rows)

    def place(index):
        within = lax.rem(index, plane)
        return {
            "row": index // plane,
            "col": within // split_count,
            "ksplit": lax.rem(within, split_count),
        }

    loads = [
        pltpu.make_async_copy(source, target, load_sem.at[at])
        for at, (source, target) in enumerate(zip(hbm_inputs, inputs))
    ]
    for load in loads:
        load.start()

    barrier = pltpu.get_barrier_semaphore()

    def greet(step, carry):
        pl.semaphore_signal(
            barrier, inc=1, device_id=place(lax.rem(me + step, devices)), device_id_type=MESH
        )
        return carry

    lax.fori_loop(1, devices, greet, 0)
    for load in loads:
        load.wait()

    positions = tile_rows * tile_cols
    state = state_ref[...].astype(F32).reshape(positions, channels)
    normed = norm_rows(state, input_gain[...], input_shift[...]).astype(BF16)
    normed_buf[...] = normed.astype(F32)
    weights = jnp.transpose(left_right[...].astype(F32)).astype(BF16)

    lane = lax.broadcasted_iota(jnp.int32, (1, LANES), 1)
    lane_block = lax.broadcasted_iota(jnp.int32, (tile_rows, LANES), 1) // tile_rows
    mask_line = mask_ref[...].astype(F32)
    mask_rows = jnp.broadcast_to(mask_line, (tile_rows, LANES))
    row_live = mask_rows
    turn = lax.rem(lane_block - my_row + row_count, row_count)
    for shift in range(1, blocks):
        row_live = jnp.where(turn == shift, pltpu.roll(mask_rows, shift * tile_rows, 1), row_live)

    lives, packs = [], []
    for quarter in range(tile_cols // blocks):
        rows = []
        col_live = jnp.zeros((tile_rows, LANES), F32)
        for inner in range(blocks):
            k = quarter * blocks + inner
            rows.append(normed_buf[pl.ds(k, tile_rows, stride=tile_cols), :])
            alive = jnp.where(lane == my_plane * tile_cols + k, mask_line, 0.0)
            alive = jnp.sum(alive, axis=1, keepdims=True)
            col_live = jnp.where(lane_block == inner, alive, col_live)
        lives.append(row_live * col_live)
        packs.append(jnp.concatenate(rows, axis=0).astype(BF16))

    def make_side(side, stage, ready):
        own = weights[side * 2 * hidden : (side + 1) * 2 * hidden]
        for quarter in range(tile_cols // blocks):
            projected = lax.dot_general(
                own, packs[quarter], (((1,), (1,)), ((), ())), preferred_element_type=F32
            )
            parts = []
            for block in range(blocks):
                at = block * tile_rows
                value = projected[at : at + tile_rows]
                gate = projected[at + hidden : at + hidden + tile_rows]
                parts.append(lives[quarter] * jax.nn.sigmoid(gate) * value)
            swapped = swap_blocks(parts, tile_rows)
            for inner in range(blocks):
                k = quarter * blocks + inner
                stage[pl.ds(k, tile_rows, stride=tile_cols), :] = swapped[inner]
        ready[...] = stage[...].reshape(ready.shape).astype(BF16)

    make_side(1, right_stage, right_send)
    pl.semaphore_wait(barrier, devices - 1)

    def right_copy(target, source, arriving):
        row = source // plane
        return pltpu.make_async_remote_copy(
            src_ref=right_send.at[:, lax.rem(target, owners)],
            dst_ref=right_recv.at[:, row, lax.rem(source, plane)],
            send_sem=right_out.at[target],
            recv_sem=right_in.at[source],
            device_id=place(source if arriving else target),
            device_id_type=MESH,
        )

    def left_copy(target, source, arriving):
        row = lax.rem(source, owners) // plane
        return pltpu.make_async_remote_copy(
            src_ref=left_send.at[:, target],
            dst_ref=left_recv.at[:, row, lax.rem(source, plane)],
            send_sem=left_out.at[target],
            recv_sem=left_in.at[lax.rem(source, owners)],
            device_id=place(my_base + (lax.rem(source, owners) if arriving else target)),
            device_id_type=MESH,
        )

    def back_copy(target, source, arriving):
        return pltpu.make_async_remote_copy(
            src_ref=back.at[target],
            dst_ref=home.at[source],
            send_sem=back_out.at[target],
            recv_sem=back_in.at[source],
            device_id=place(my_base + (source if arriving else target)),
            device_id_type=MESH,
        )

    far_base = owners - my_base

    def send_far(step, carry):
        right_copy(far_base + lax.rem(my_group + step, owners), me, False).start()
        return carry

    def send_near(step, carry):
        right_copy(my_base + lax.rem(my_group + step, owners), me, False).start()
        return carry

    def send_left(step, carry):
        left_copy(lax.rem(my_group + step, owners), me, False).start()
        return carry

    lax.fori_loop(0, owners, send_far, 0)
    lax.fori_loop(1, owners, send_near, 0)
    right_recv[:, my_row, my_plane] = right_send[:, my_group]
    make_side(0, left_stage, left_send)
    lax.fori_loop(1, owners, send_left, 0)
    left_recv[:, my_inner, my_plane] = left_send[:, my_group]
    gates = jnp.dot(normed, output_gate[...], preferred_element_type=F32)
    gate_buf[...] = jax.nn.sigmoid(gates)

    def wait_left(step, carry):
        source = lax.rem(my_group + owners - step, owners)
        left_copy(source, source, True).wait_recv()
        return carry

    lax.fori_loop(1, owners, wait_left, 0)

    depth = plane * tile_cols
    half_bit = (lax.broadcasted_iota(jnp.int32, (tile_rows, LANES), 1) // tile_cols) & 1
    lefts = []
    for bit in range(2):
        both = [
            jnp.transpose(left_recv[bit, inner].reshape(depth, LANES).astype(F32))
            for inner in range(half_rows)
        ]
        lefts.append(jnp.concatenate(both, axis=0).astype(BF16))

    for turn in range(row_count):
        if turn < half_rows:
            row = my_base // plane + lax.rem(my_inner + turn, half_rows)
        else:
            row = far_base // plane + lax.rem(my_inner + turn, half_rows)

        def wait_right(step, carry):
            source = row * plane + lax.rem(my_plane + step, plane)
            right_copy(source, source, True).wait_recv()
            return carry

        lax.fori_loop(1 if turn == 0 else 0, plane, wait_right, 0)
        products = [
            jnp.dot(
                lefts[bit], right_recv[bit, row].reshape(depth, LANES), preferred_element_type=F32
            )
            for bit in range(2)
        ]
        for inner in range(half_rows):
            mixed = []
            for product in products:
                piece = product[inner * LANES : (inner + 1) * LANES]
                chosen = piece[:tile_rows]
                for block in range(1, blocks):
                    chosen = jnp.where(
                        lane_block == block,
                        piece[block * tile_rows : (block + 1) * tile_rows],
                        chosen,
                    )
                mixed.append(chosen)
            first = jnp.where(half_bit == 0, mixed[0], pltpu.roll(mixed[1], tile_cols, 1))
            second = jnp.where(
                half_bit == 1, mixed[1], pltpu.roll(mixed[0], LANES - tile_cols, 1)
            )
            for half, part in ((0, first), (1, second)):
                target = inner * plane + row * 2 + half
                back[target] = part.astype(BACK)

                @pl.when(target != my_group)
                def _():
                    back_copy(target, my_group, False).start()

                @pl.when(target == my_group)
                def _():
                    home[my_group] = back[my_group]

    def wait_back(step, carry):
        source = lax.rem(my_group + owners - step, owners)
        back_copy(source, source, True).wait_recv()
        return carry

    lax.fori_loop(1, owners, wait_back, 0)

    left_stage[...] = home[...].astype(F32).reshape(owners * tile_rows, LANES)
    step_rows = LANES // tile_cols
    for group in range(tile_rows // step_rows):
        rows = [
            left_stage[pl.ds(group * step_rows + at, owners, stride=tile_rows), :]
            for at in range(step_rows)
        ]
        turned = jnp.transpose(jnp.concatenate(rows, axis=0))
        parts = [turned[b * tile_cols : (b + 1) * tile_cols] for b in range(step_rows)]
        together = jnp.concatenate(swap_blocks(parts, owners), axis=0)
        normed_out = norm_rows(together, final_gain[...], final_shift[...]).astype(BF16)
        projected_out = jnp.dot(normed_out, output_weight[...], preferred_element_type=F32)
        gated = gate_buf[group * LANES : (group + 1) * LANES] * projected_out
        out_ref[group * step_rows : (group + 1) * step_rows] = gated.reshape(
            step_rows, tile_cols, channels
        ).astype(BF16)

    def drain_near(step, carry):
        target = lax.rem(my_group + step, owners)
        right_copy(my_base + target, me, False).wait_send()
        left_copy(target, me, False).wait_send()
        back_copy(target, my_group, False).wait_send()
        return carry

    def drain_far(step, carry):
        right_copy(far_base + lax.rem(my_group + step, owners), me, False).wait_send()
        return carry

    lax.fori_loop(1, owners, drain_near, 0)
    lax.fori_loop(0, owners, drain_far, 0)


def fused(sizes, *arrays):
    row_count, col_count, split_count, tile_rows, tile_cols, channels, hidden = sizes
    plane = col_count * split_count
    devices = row_count * plane
    owners = devices // 2
    state, *lines, weights, gate, gain_out, shift_out, weight_out = arrays
    lines = [line[None] for line in lines]
    operands = [state, *lines, weights, gate, gain_out[None], shift_out[None], weight_out]
    flat = (tile_rows * tile_cols, LANES)
    tile = (tile_cols, LANES)
    counts = (len(operands), owners, owners, devices, devices, owners, owners)
    return pl.pallas_call(
        functools.partial(kernel, sizes),
        out_shape=pltpu.VMEM(state.shape, BF16),
        in_specs=[pl.BlockSpec(memory_space=pl.ANY)] * len(operands),
        out_specs=pl.BlockSpec(memory_space=pltpu.VMEM),
        scratch_shapes=[pltpu.VMEM(item.shape, item.dtype) for item in operands]
        + [pltpu.VMEM(flat, F32)] * 4
        + [pltpu.VMEM((2, owners) + tile, BF16)] * 2
        + [
            pltpu.VMEM((2, row_count // 2, plane) + tile, BF16),
            pltpu.VMEM((2, row_count, plane) + tile, BF16),
            pltpu.VMEM((owners, tile_rows, LANES), BACK),
            pltpu.VMEM((owners, tile_rows, LANES), BACK),
        ]
        + [pltpu.SemaphoreType.DMA((count,)) for count in counts],
        compiler_params=pltpu.CompilerParams(collective_id=0, has_side_effects=True),
    )(*operands)


def update(*arrays):
    state, mask, weight_out = arrays[0], arrays[1], arrays[8]
    tile_rows, tile_cols, channels = state.shape
    hidden = weight_out.shape[0]
    row_count, col_count = lax.axis_size("row"), lax.axis_size("col")
    split_count = lax.axis_size("ksplit")
    devices = row_count * col_count * split_count
    fits = (
        channels == LANES
        and hidden == LANES
        and mask.shape[0] == LANES
        and row_count * tile_rows == LANES
        and devices == tile_rows
        and row_count % 2 == 0
        and devices // 2 == tile_cols
        and tile_rows == 2 * tile_cols
        and tile_cols % 16 == 0
    )
    if fits:
        sizes = (row_count, col_count, split_count, tile_rows, tile_cols, channels, hidden)
        return fused(sizes, *arrays)
    return body(*arrays)


def norm_over(data, norm_gain, norm_shift, over_axis):
    average = jnp.mean(data, axis=over_axis, keepdims=True)
    centred = data - average
    spread = jnp.mean(centred * centred, axis=over_axis, keepdims=True)
    return centred * lax.rsqrt(spread + 1e-05) * norm_gain + norm_shift


def gated_side(normed_in, weights, live_mask, hidden):
    values = jnp.einsum(
        "ikc,ch->hik", normed_in, weights[:, :hidden], preferred_element_type=jnp.float32
    )
    gates = jnp.einsum(
        "ikc,ch->hik", normed_in, weights[:, hidden:], preferred_element_type=jnp.float32
    )
    return (live_mask * jax.nn.sigmoid(gates) * values).astype(jnp.bfloat16)


def contract_parts(left_parts, right_parts, row_count, col_count):
    count_items = left_parts.shape[2]
    tile_rows = left_parts.shape[3]
    tile_cols = left_parts.shape[4]

    def assemble(parts):
        return parts.transpose(2, 0, 3, 1, 4).reshape(
            count_items, row_count * tile_rows, col_count * tile_cols
        )

    products = jnp.einsum(
        "cik,cjk->cij",
        assemble(left_parts),
        assemble(right_parts),
        preferred_element_type=jnp.float32,
    )
    returned = products.reshape(count_items, row_count, tile_rows, col_count, tile_cols)
    return returned.transpose(1, 3, 0, 2, 4)


def body(
    pair_state,
    residue_mask,
    input_gain,
    input_shift,
    left_right,
    output_gate,
    final_gain,
    final_shift,
    output_weight,
):
    tile_rows, tile_cols, channels = pair_state.shape
    hidden = output_weight.shape[0]
    normed_in = norm_over(pair_state.astype(jnp.float32), input_gain, input_shift, 2).astype(
        jnp.bfloat16
    )
    row_start = lax.axis_index("row") * tile_rows
    col_start = lax.axis_index(("col", "ksplit")) * tile_cols
    row_live = lax.dynamic_slice_in_dim(residue_mask, row_start, tile_rows).astype(jnp.float32)
    col_live = lax.dynamic_slice_in_dim(residue_mask, col_start, tile_cols).astype(jnp.float32)
    live_mask = row_live[:, None] * col_live[None, :]
    left_side = gated_side(normed_in, left_right[:, : 2 * hidden], live_mask, hidden)
    right_side = gated_side(normed_in, left_right[:, 2 * hidden :], live_mask, hidden)
    devices_all = lax.axis_size(("row", "col", "ksplit"))
    row_count = lax.axis_size("row")
    col_count = devices_all // row_count
    per_device = hidden // devices_all
    grouped_left = left_side.reshape(devices_all, per_device, tile_rows, tile_cols)
    grouped_right = right_side.reshape(devices_all, per_device, tile_rows, tile_cols)
    left_parts = lax.all_to_all(
        grouped_left, ("row", "col", "ksplit"), split_axis=0, concat_axis=0, tiled=True
    )
    right_parts = lax.all_to_all(
        grouped_right, ("row", "col", "ksplit"), split_axis=0, concat_axis=0, tiled=True
    )
    count_items = left_parts.shape[1]
    shaped_left = left_parts.reshape(row_count, col_count, count_items, tile_rows, tile_cols)
    shaped_right = right_parts.reshape(row_count, col_count, count_items, tile_rows, tile_cols)
    returned = contract_parts(shaped_left, shaped_right, row_count, col_count)
    returned = returned.reshape(devices_all, count_items, tile_rows, tile_cols)
    received = lax.all_to_all(
        returned, ("row", "col", "ksplit"), split_axis=0, concat_axis=0, tiled=True
    )
    mixed_tile = received.reshape(hidden, tile_rows, tile_cols)
    normed_out = norm_over(
        mixed_tile, final_gain[:, None, None], final_shift[:, None, None], 0
    ).astype(jnp.bfloat16)
    projected_out = jnp.einsum(
        "hij,hc->ijc", normed_out, output_weight, preferred_element_type=jnp.float32
    )
    gate_values = jax.nn.sigmoid(
        jnp.einsum("ijc,cd->ijd", normed_in, output_gate, preferred_element_type=jnp.float32)
    )
    return (gate_values * projected_out).astype(jnp.bfloat16)


def solution(mesh):
    placed = (
        P(("groups", "row"), ("col", "ksplit"), None),
        P("groups"),
        P(),
        P(),
        P(),
        P(),
        P(),
        P(),
        P(),
    )
    return jax.shard_map(
        update,
        mesh=mesh,
        in_specs=placed,
        out_specs=P(("groups", "row"), ("col", "ksplit"), None),
        check_vma=False,
    )
```
